256 devices in a mesh: blk: 64 (over z, y_hi, x), deg: 4 (over y_lo, core).
Axes of the slice: x: 4, y: 4 (y_hi: 2, y_lo: 2; y = y_hi * 2 + y_lo), z: 8, core: 2. Of those that a mesh axis runs over, the one named last changes fastest.
Arguments:
- source: bfloat16 [672, 16384], P('deg', 'blk'), may hold values from -6 to 6
- operators: bfloat16 [12, 672, 672], replicated, may hold values from -0.125 to 0.125
- mie_factor: float32 [672, 16384], P('deg', 'blk'), may hold values from 0.3 to 1.5
- pair_source: int32 [6, 4, 16384], P(None, None, 'blk'), may hold values from 0 to 255
- pair_class: int32 [6, 4, 16384], P(None, None, 'blk'), may hold values from 0 to 11
- pair_scale: bfloat16 [6, 4, 16384], P(None, None, 'blk'), may hold values from 0.25 to 1
Outputs:
- result: float32 [672, 16384], P('deg', 'blk')
The draws below stay inside these ranges and needn't reach their ends.
Inputs may be any that keep to these rules, and one draw needn't show every extreme that they name: `pair_source`: index of a source sphere within the visited block.
All inputs are finite; a program needn't handle non-finite values.
Results may differ from the reference program's by a relative error of at most 0.0075.
Values may be sent and summed in bfloat16 or wider, within the bound.
No kernel may reach another device: no remote copies, remote signals or barrier semaphores. Data moves between devices by JAX's collectives and lax.ppermute only.
A program may use at most 64 MiB of HBM per device.

```python
import math
import jax
import jax.numpy as jnp
from jax import lax

COEF = 672
NDIR = 12
PAIRS = 4
STEPS = 6
SPH_DEV = 256
SPHERES = 16384
N_BLK = 64


def place_ends(entries, key, low, high):
    shape = entries.shape
    place = [jax.random.randint(jax.random.fold_in(key, axis), (), 0, shape[axis]) for axis in range(len(shape))]
    entries = entries.at[tuple(place)].set(low)
    longest = shape.index(max(shape))
    place[longest] = (place[longest] + 1) % shape[longest]
    return entries.at[tuple(place)].set(high)


def block_levels(key, dims, shards, low, top_value):
    loudness, own = 1.0, jax.random.fold_in(key, 6)
    for axis_at, shards_of in shards:
        heights = jnp.exp(jax.random.uniform(jax.random.fold_in(own, axis_at), (shards_of,), jnp.float32, low / len(shards), top_value / len(shards)))
        loudness = loudness * jnp.repeat(heights, dims[axis_at] // shards_of).reshape([-1 if axis == axis_at else 1 for axis in range(len(dims))])
    return loudness


def bell_draw(own_key, dims, deviation, most, cuts=(), kind=jnp.bfloat16):
    result = jax.random.normal(own_key, dims, jnp.float32) * deviation
    if len(cuts) > 0:
        result = block_levels(own_key, dims, cuts, -0.22, 0.18) * result
    return jnp.clip(result, min=-most, max=most).astype(kind)


def setup_inputs(seed: int = 0) -> dict:
    key_of = jax.random.split(jax.random.key(seed), 7)
    return {
        "source": bell_draw(key_of[0], (COEF, SPHERES), 1.0, 6.0, ((0, 4), (1, 64))),
        "operators": bell_draw(key_of[1], (NDIR, COEF, COEF), (COEF * PAIRS) ** -0.5, 0.125),
        "mie_factor": jnp.clip(jnp.exp(math.log(1.5) - 1.60943787 * jax.random.uniform(key_of[2], (COEF, SPHERES), jnp.float32) ** block_levels(key_of[2], (COEF, SPHERES), ((0, 4), (1, 64)), -0.2, 0.2)), 0.3, 1.5),
        "pair_source": place_ends(jax.random.randint(key_of[3], (STEPS, PAIRS, SPHERES), 0, SPH_DEV), jax.random.fold_in(key_of[3], 1), 0, SPH_DEV - 1).astype(jnp.int32),
        "pair_class": place_ends(jax.random.randint(key_of[4], (STEPS, PAIRS, SPHERES), 0, NDIR), jax.random.fold_in(key_of[4], 1), 0, NDIR - 1).astype(jnp.int32),
        "pair_scale": jnp.clip(jnp.exp(math.log(1.0) - 1.3862944 * jax.random.uniform(key_of[5], (STEPS, PAIRS, SPHERES), jnp.float32) ** block_levels(key_of[5], (STEPS, PAIRS, SPHERES), ((2, 64),), -0.2, 0.2)), 0.25, 1.0).astype(jnp.bfloat16),
    }


def combine(visiting, indices, kinds, scales, classes):
    picked = jnp.take(visiting, indices, axis=1).astype(jnp.float32)
    onehot = kinds[:, None, :] == jnp.arange(classes, dtype=jnp.int32)[None, :, None]
    weights = jnp.where(onehot, scales[:, None, :], jnp.zeros_like(scales[:, None, :])).astype(jnp.float32)
    gathered = jnp.einsum("rki,kci->cri", picked, weights)
    return gathered.astype(jnp.bfloat16).reshape(classes * visiting.shape[0], visiting.shape[1])


def reference(source, operators, mie_factor, pair_source, pair_class, pair_scale):
    blocks = source.reshape(COEF, N_BLK, SPH_DEV)
    weight_flat = jnp.transpose(operators, (1, 0, 2)).reshape(COEF, NDIR * COEF)

    def one_block(block_index):
        target_field = jnp.zeros((COEF, SPH_DEV), jnp.float32)
        offset_start = (block_index * SPH_DEV).astype(jnp.int32)
        for cycle_step in range(STEPS):
            anchor = ((block_index - cycle_step) % N_BLK).astype(jnp.int32)
            visiting = lax.dynamic_index_in_dim(blocks, anchor, 1, keepdims=False)
            indices = lax.dynamic_slice_in_dim(pair_source[cycle_step], offset_start, SPH_DEV, 1)
            kinds = lax.dynamic_slice_in_dim(pair_class[cycle_step], offset_start, SPH_DEV, 1)
            scales = lax.dynamic_slice_in_dim(pair_scale[cycle_step], offset_start, SPH_DEV, 1)
            combined = combine(visiting, indices, kinds, scales, NDIR)
            target_field = target_field + jnp.dot(weight_flat, combined, preferred_element_type=jnp.float32)
        return target_field

    fields = lax.map(one_block, jnp.arange(N_BLK, dtype=jnp.int32))
    target_field = jnp.transpose(fields, (1, 0, 2)).reshape(COEF, SPHERES)
    return source.astype(jnp.float32) - mie_factor * target_field
```

```python
import functools

import jax
import jax.numpy as jnp
from jax import lax
from jax.experimental import pallas as pl
from jax.experimental.pallas import tpu as pltpu
from jax.sharding import PartitionSpec as P

VMEM = pl.BlockSpec(memory_space=pltpu.VMEM)


def prepare(position, operators, sources, kinds, scales, table, weights, stage, arrived):
    classes, full, _ = operators.shape
    visits, slots, spheres = sources.shape
    rows = weights.shape[2]
    deg = position[0]
    for c in range(classes):
        pltpu.make_async_copy(operators.at[c], stage.at[c], arrived.at[c]).start()

    sphere = lax.broadcasted_iota(jnp.int32, (spheres, spheres), 0).astype(jnp.float32).astype(jnp.bfloat16)

    def visit(s, _):
        picked = sources[s].astype(jnp.float32).astype(jnp.bfloat16)
        kind = kinds[s]
        scale = scales[s]
        zero = jnp.zeros((), jnp.bfloat16)
        hits = [
            jnp.where(sphere == picked[k : k + 1, :], scale[k : k + 1, :], zero) for k in range(slots)
        ]
        for c in range(classes):
            own = jnp.where(kind == c, 1.0, 0.0).astype(jnp.bfloat16)
            terms = [hits[k] * own[k : k + 1, :] for k in range(slots)]
            while len(terms) > 1:
                terms = [sum(terms[i + 1 : i + 2], terms[i]) for i in range(0, len(terms), 2)]
            table[c, s] = terms[0]
        return 0

    lax.fori_loop(0, visits, visit, 0)

    row = lax.broadcasted_iota(jnp.int32, (full, rows), 0)
    column = lax.broadcasted_iota(jnp.int32, (full, rows), 1)
    pick = jnp.where(row == column + deg * rows, 1.0, 0.0).astype(jnp.bfloat16)

    def operator(c, _):
        pltpu.make_async_copy(operators.at[c], stage.at[c], arrived.at[c]).wait()
        own = jnp.dot(stage[c], pick, preferred_element_type=jnp.float32)
        for d in range(full // rows):
            weights[c, jnp.bitwise_xor(deg, d)] = own[d * rows : (d + 1) * rows].astype(jnp.bfloat16)
        return 0

    lax.fori_loop(0, classes, operator, 0)


def interact(groups, *refs):
    visiting, table, weights = refs[:-6], refs[-6], refs[-5]
    outs = refs[-4:]
    classes = table.shape[0]
    combined = []
    for c in range(classes):
        mixed = jnp.dot(visiting[0][...], table[c, 0], preferred_element_type=jnp.float32)
        for s in range(1, len(visiting)):
            mixed += jnp.dot(visiting[s][...], table[c, s], preferred_element_type=jnp.float32)
        combined.append(mixed.astype(jnp.bfloat16))
    for d in range(groups - 1, -1, -1):
        field = jnp.dot(weights[0, d], combined[0], preferred_element_type=jnp.float32)
        for c in range(1, classes):
            field += jnp.dot(weights[c, d], combined[c], preferred_element_type=jnp.float32)
        outs[d][...] = field.astype(outs[d].dtype)


def local(source, operators, mie_factor, pair_source, pair_class, pair_scale):
    rows, spheres = source.shape
    classes, full, _ = operators.shape
    visits = pair_source.shape[0]
    groups = full // rows
    blocks = lax.axis_size("blk")
    visiting = [source]
    for s in range(1, visits):
        visiting.append(lax.ppermute(source, "blk", [(b, (b + s) % blocks) for b in range(blocks)]))

    position = jnp.asarray(lax.axis_index("deg"), jnp.int32).reshape(1)
    table, weights = pl.pallas_call(
        prepare,
        out_shape=(
            jax.ShapeDtypeStruct((classes, visits, spheres, spheres), jnp.bfloat16),
            jax.ShapeDtypeStruct((classes, groups, rows, rows), jnp.bfloat16),
        ),
        in_specs=[pl.BlockSpec(memory_space=pltpu.SMEM), pl.BlockSpec(memory_space=pltpu.HBM)] + [VMEM] * 3,
        out_specs=(VMEM, VMEM),
        scratch_shapes=[
            pltpu.VMEM((classes, full, full), jnp.bfloat16),
            pltpu.SemaphoreType.DMA((classes,)),
        ],
        compiler_params=pltpu.CompilerParams(vmem_limit_bytes=24 * 2**20),
        cost_estimate=pl.CostEstimate(
            flops=2 * classes * full * full * rows, bytes_accessed=2 * operators.size, transcendentals=0
        ),
        name="prepare",
    )(position, operators, pair_source, pair_class, pair_scale)

    outs = pl.pallas_call(
        functools.partial(interact, groups),
        out_shape=(jax.ShapeDtypeStruct((rows, spheres), jnp.float32),)
        + (jax.ShapeDtypeStruct((rows, spheres), jnp.bfloat16),) * (groups - 1),
        in_specs=[VMEM] * (visits + 2),
        out_specs=(VMEM,) * groups,
        compiler_params=pltpu.CompilerParams(vmem_limit_bytes=24 * 2**20),
        cost_estimate=pl.CostEstimate(
            flops=2 * rows * spheres * classes * (visits * spheres + full), bytes_accessed=2 * table.size, transcendentals=0
        ),
        name="interact",
    )(*visiting, table, weights)

    field = outs[0]
    for d in range(1, groups):
        other = lax.ppermute(outs[d], "deg", [(i, i ^ d) for i in range(groups)])
        field = field + other.astype(jnp.float32)
    return source.astype(jnp.float32) - mie_factor * field


def solution(mesh):
    return jax.shard_map(
        local,
        mesh=mesh,
        in_specs=(
            P("deg", "blk"),
            P(),
            P("deg", "blk"),
            P(None, None, "blk"),
            P(None, None, "blk"),
            P(None, None, "blk"),
        ),
        out_specs=P("deg", "blk"),
        check_vma=False,
    )
```

```python
import functools

import jax
import jax.numpy as jnp
from jax import lax
from jax.experimental import pallas as pl
from jax.experimental.pallas import tpu as pltpu
from jax.sharding import PartitionSpec as P


LANES = 128
STRIP = 32
EARLY = 4
SPHERE_BITS = 8
SCALE_BITS = 10
SCALE_UNIT = 512
VMEM = pl.BlockSpec(memory_space=pltpu.VMEM)


def prepare(codes, operators, table, weights, stage, arrived):
    classes, full, _ = operators.shape
    visits, slots, spheres = codes.shape
    rows = weights.shape[2]
    deg = lax.axis_index("deg")
    first = [d * rows // LANES * LANES for d in range(full // rows)]
    width = [min(-(-((d + 1) * rows - first[d]) // LANES) * LANES, full - first[d]) for d in range(full // rows)]

    def window(d, c):
        source, target = operators.at[c], stage.at[c]
        if width[d] % LANES == 0:
            source, target = (ref.at[:, first[d] : first[d] + width[d]] for ref in (source, target))
        return pltpu.make_async_copy(source, target, arrived.at[c])

    def each_group(body):
        for d in range(full // rows):
            pl.when(deg == d)(functools.partial(body, d))

    def fetch(d):
        for c in range(classes):
            window(d, c).start()

    each_group(fetch)

    def spread(x, k):
        return jnp.broadcast_to(x[k : k + 1, :], (STRIP, spheres))

    zero = jnp.zeros((), jnp.bfloat16)
    sphere = lax.broadcasted_iota(jnp.int32, (STRIP, spheres), 0).astype(jnp.float32).astype(jnp.bfloat16)

    def tables(s, before, after):
        kind = jnp.right_shift(codes[s], SPHERE_BITS + SCALE_BITS)
        picked = jnp.bitwise_and(jnp.right_shift(codes[s], SCALE_BITS), 2**SPHERE_BITS - 1)
        scale = jnp.bitwise_and(codes[s], 2**SCALE_BITS - 1).astype(jnp.float32) * (1.0 / SCALE_UNIT)
        picked, scale = picked.astype(jnp.float32).astype(jnp.bfloat16), scale.astype(jnp.bfloat16)
        picked = [spread(picked, k) for k in range(slots)]
        scale = [spread(scale, k) for k in range(slots)]
        mine = []
        for c in range(classes):
            flags = jnp.where(kind == c, 1.0, 0.0).astype(jnp.bfloat16)
            mine.append([spread(flags, k) for k in range(slots)])
        for turn, start in enumerate(range(0, spheres, STRIP)):
            work = before(turn)
            here = sphere + jnp.asarray(start, jnp.bfloat16)
            hits = [jnp.where(here == picked[k], scale[k], zero) for k in range(slots)]
            for c in range(classes):
                terms = [hits[k] * mine[c][k] for k in range(slots)]
                while len(terms) > 1:
                    terms = [sum(terms[i + 1 : i + 2], terms[i]) for i in range(0, len(terms), 2)]
                table[c, s, start : start + STRIP] = terms[0]
            after(work)

    def with_operators(d):
        row = lax.broadcasted_iota(jnp.int32, (width[d], rows), 0)
        column = lax.broadcasted_iota(jnp.int32, (width[d], rows), 1)
        pick = jnp.where(row == column + (d * rows - first[d]), 1.0, 0.0).astype(jnp.bfloat16)
        groups, turns = full // rows, spheres // STRIP
        share = classes // (visits - 2)

        def visit(s, _):
            base = (s - 1) * share
            for c in range(share):
                window(d, base + c).wait()

            def before(turn):
                done = []
                for chunk in range(turn * share * groups // turns, (turn + 1) * share * groups // turns):
                    c, g = base + chunk // groups, chunk % groups
                    part = stage[c, g * rows : (g + 1) * rows, first[d] : first[d] + width[d]]
                    done.append((c, g ^ d, jnp.dot(part, pick, preferred_element_type=jnp.float32)))
                return done

            def after(done):
                for c, slot, columns in done:
                    weights[c, slot] = columns.astype(jnp.bfloat16)

            tables(s, before, after)
            return 0

        lax.fori_loop(1, visits - 1, visit, 0)

    tables(0, lambda _: None, lambda _: None)
    each_group(with_operators)
    tables(visits - 1, lambda _: None, lambda _: None)


def add_visits(start, visiting, table, first_visit, c):
    for i, block in enumerate(visiting):
        term = jnp.dot(block[...], table[c, first_visit + i], preferred_element_type=jnp.float32)
        start = term if start is None else start + term
    return start


def gather_early(*refs):
    *visiting, table, early = refs
    for c in range(table.shape[0]):
        early[c] = add_visits(None, visiting, table, 0, c)


def field_of(weights, combined, slot):
    field = None
    for c in range(weights.shape[0]):
        term = jnp.dot(weights[c, slot], combined[c], preferred_element_type=jnp.float32)
        field = term if field is None else field + term
    return field


def interact_far(early_visits, slots, *refs):
    early, *visiting, table, weights, combined = refs[: len(refs) - len(slots)]
    mixed = []
    for c in range(table.shape[0]):
        mixed.append(add_visits(early[c], visiting, table, early_visits, c).astype(jnp.bfloat16))
        combined[c] = mixed[c]
    for slot, out in zip(slots, refs[len(refs) - len(slots) :]):
        out[...] = field_of(weights, mixed, slot).astype(out.dtype)


def interact_near(slots, weights, combined, *outs):
    for slot, out in zip(slots, outs):
        out[...] = field_of(weights, combined, slot).astype(out.dtype)


def local(source, operators, mie_factor, pair_source, pair_class, pair_scale):
    rows, spheres = source.shape
    classes, full, _ = operators.shape
    visits = pair_source.shape[0]
    groups = full // rows
    blocks = lax.axis_size("blk")
    visiting = [source]
    for s in range(1, visits):
        visiting.append(lax.ppermute(source, "blk", [(b, (b + s) % blocks) for b in range(blocks)]))

    units = (pair_scale.astype(jnp.float32) * SCALE_UNIT).astype(jnp.int32)
    codes = (pair_class * 2**SPHERE_BITS + pair_source) * 2**SCALE_BITS + units
    table, weights = pl.pallas_call(
        prepare,
        out_shape=(
            jax.ShapeDtypeStruct((classes, visits, spheres, spheres), jnp.bfloat16),
            jax.ShapeDtypeStruct((classes, groups, rows, rows), jnp.bfloat16),
        ),
        in_specs=[VMEM, pl.BlockSpec(memory_space=pl.ANY)],
        out_specs=(VMEM, VMEM),
        scratch_shapes=[
            pltpu.VMEM((classes, full, full), jnp.bfloat16),
            pltpu.SemaphoreType.DMA((classes,)),
        ],
        compiler_params=pltpu.CompilerParams(vmem_limit_bytes=40 * 2**20),
        cost_estimate=pl.CostEstimate(
            flops=2 * classes * full * full * rows, bytes_accessed=2 * operators.size, transcendentals=0
        ),
        name="prepare",
    )(codes, operators)

    def call(kernel, out_shape, flops, *operands):
        return pl.pallas_call(
            kernel,
            out_shape=out_shape,
            in_specs=[VMEM] * len(operands),
            out_specs=jax.tree.map(lambda _: VMEM, out_shape),
            compiler_params=pltpu.CompilerParams(vmem_limit_bytes=16 * 2**20),
            cost_estimate=pl.CostEstimate(flops=flops, bytes_accessed=2 * source.size, transcendentals=0),
        )(*operands)

    def shape(dtype, *lead):
        return jax.ShapeDtypeStruct((*lead, rows, spheres), dtype)

    gather = 2 * rows * spheres * spheres * classes
    product = 2 * rows * rows * spheres * classes
    late = max(visits - EARLY, 0)
    early = call(gather_early, shape(jnp.float32, classes), (visits - late) * gather, *visiting[:EARLY], table)
    far, near = (3, 2), (1, 0)
    combined, *sent = call(
        functools.partial(interact_far, EARLY, far),
        (shape(jnp.bfloat16, classes),) + (shape(jnp.bfloat16),) * len(far),
        late * gather + len(far) * product,
        early,
        *visiting[EARLY:],
        table,
        weights,
    )
    others = []
    for d, x in zip(far, sent):
        others.append(lax.ppermute(x, "deg", [(i, i ^ d) for i in range(groups)]))
    sent, field = call(
        functools.partial(interact_near, near),
        (shape(jnp.bfloat16), shape(jnp.float32)),
        len(near) * product,
        weights,
        combined,
    )
    others.append(lax.ppermute(sent, "deg", [(i, i ^ 1) for i in range(groups)]))
    for other in others:
        field = field + other.astype(jnp.float32)
    return source.astype(jnp.float32) - mie_factor * field


def solution(mesh):
    return jax.shard_map(
        local,
        mesh=mesh,
        in_specs=(
            P("deg", "blk"),
            P(),
            P("deg", "blk"),
            P(None, None, "blk"),
            P(None, None, "blk"),
            P(None, None, "blk"),
        ),
        out_specs=P("deg", "blk"),
        check_vma=False,
    )
```

```python
import functools

import jax
import jax.numpy as jnp
from jax import lax
from jax.experimental import pallas as pl
from jax.experimental.pallas import tpu as pltpu
from jax.sharding import PartitionSpec as P


LANES = 128
STRIP = 32
EARLY = 4
SPHERE_BITS = 8
SCALE_BITS = 10
SCALE_UNIT = 512
DEPTH = 256
LEAD = 8
VMEM = pl.BlockSpec(memory_space=pltpu.VMEM)


def column_windows(full, rows):
    windows = []
    for d in range(full // rows):
        start = d * rows // LANES * LANES
        if (d + 1) * rows - start > DEPTH:
            start += LANES
        windows.append((start, min(DEPTH, full - start), d * rows - start))
        assert windows[-1][2] >= -LEAD and windows[-1][2] % 8 == 0
    return windows


def prepare(codes, operators, table, weights, extra, stage, arrived):
    classes, full, _ = operators.shape
    visits, slots, spheres = codes.shape
    rows = full // lax.axis_size("deg")
    deg = lax.axis_index("deg")
    windows = column_windows(full, rows)

    def window(d, c):
        start, length, _ = windows[d]
        if length == DEPTH:
            return pltpu.make_async_copy(operators.at[c, :, start : start + length], weights.at[c], arrived.at[c])
        return pltpu.make_async_copy(operators.at[c], stage.at[c], arrived.at[c])

    def each_group(body):
        for d in range(full // rows):
            pl.when(deg == d)(functools.partial(body, d))

    def fetch(d):
        for c in range(classes):
            window(d, c).start()

    each_group(fetch)

    def spread(x, k):
        return jnp.broadcast_to(x[k : k + 1, :], (STRIP, spheres))

    zero = jnp.zeros((), jnp.bfloat16)
    sphere = lax.broadcasted_iota(jnp.int32, (STRIP, spheres), 0).astype(jnp.float32).astype(jnp.bfloat16)

    def tables(s, _):
        kind = jnp.right_shift(codes[s], SPHERE_BITS + SCALE_BITS)
        picked = jnp.bitwise_and(jnp.right_shift(codes[s], SCALE_BITS), 2**SPHERE_BITS - 1)
        scale = jnp.bitwise_and(codes[s], 2**SCALE_BITS - 1).astype(jnp.float32) * (1.0 / SCALE_UNIT)
        picked, scale = picked.astype(jnp.float32).astype(jnp.bfloat16), scale.astype(jnp.bfloat16)
        picked = [spread(picked, k) for k in range(slots)]
        scale = [spread(scale, k) for k in range(slots)]
        mine = []
        for c in range(classes):
            flags = jnp.where(kind == c, 1.0, 0.0).astype(jnp.bfloat16)
            mine.append([spread(flags, k) for k in range(slots)])
        for start in range(0, spheres, STRIP):
            here = sphere + jnp.asarray(start, jnp.bfloat16)
            hits = [jnp.where(here == picked[k], scale[k], zero) for k in range(slots)]
            for c in range(classes):
                terms = [hits[k] * mine[c][k] for k in range(slots)]
                while len(terms) > 1:
                    terms = [sum(terms[i + 1 : i + 2], terms[i]) for i in range(0, len(terms), 2)]
                table[c, s, start : start + STRIP] = terms[0]
        return 0

    lax.fori_loop(0, visits, tables, 0)

    def finish(d):
        start, length, first_row = windows[d]
        whole = length // LANES * LANES
        row = lax.broadcasted_iota(jnp.int32, (LANES, extra.shape[1]), 0) - (LANES + first_row)
        column = lax.broadcasted_iota(jnp.int32, (LANES, extra.shape[1]), 1)
        before = None
        for c in range(classes):
            window(d, c).wait()
            if length < DEPTH:
                weights[c, :, :whole] = stage[c, :, start : start + whole]
                weights[c, :, whole:] = jnp.zeros((full, DEPTH - whole), jnp.bfloat16)
                weights[c, :, whole:length] = stage[c, :, start + whole : start + length]
            if first_row < 0:
                pick = jnp.where((row >= 0) & (row + LEAD * c == column), 1.0, 0.0).astype(jnp.bfloat16)
                term = jnp.dot(stage[c, :, start - LANES : start], pick, preferred_element_type=jnp.float32)
                before = term if before is None else before + term
        extra[...] = jnp.zeros_like(extra) if before is None else before.astype(jnp.bfloat16)

    each_group(finish)


def add_visits(start, visiting, table, first_visit, c):
    for i, block in enumerate(visiting):
        term = jnp.dot(block[...], table[c, first_visit + i], preferred_element_type=jnp.float32)
        start = term if start is None else start + term
    return start


def gather_early(*refs):
    *visiting, table, early = refs
    for c in range(table.shape[0]):
        early[c] = add_visits(None, visiting, table, 0, c)


def field_of(weights, extra, combined, slot):
    rows = extra.shape[0] // lax.axis_size("deg")
    chunk = pl.ds(pl.multiple_of(jnp.bitwise_xor(lax.axis_index("deg"), slot) * rows, 8), rows)
    lead = jnp.concatenate([combined[c, :LEAD] for c in range(weights.shape[0])], axis=0)
    field = jnp.dot(extra[chunk], lead, preferred_element_type=jnp.float32)
    for c in range(weights.shape[0]):
        field += jnp.dot(weights[c, chunk], combined[c, LEAD:], preferred_element_type=jnp.float32)
    return field


def interact_far(early_visits, slots, *refs):
    early, *visiting, table, weights, extra, combined = refs[: len(refs) - len(slots)]
    rows = early.shape[1]
    place = jnp.int32(LEAD)
    for d, (_, _, first_row) in enumerate(column_windows(weights.shape[1], rows)):
        place += jnp.where(lax.axis_index("deg") == d, first_row, 0)
    combined[...] = jnp.zeros_like(combined)
    for c in range(table.shape[0]):
        mixed = add_visits(early[c], visiting, table, early_visits, c)
        combined[c, pl.ds(pl.multiple_of(place, 8), rows)] = mixed.astype(jnp.bfloat16)
    for slot, out in zip(slots, refs[len(refs) - len(slots) :]):
        out[...] = field_of(weights, extra, combined, slot).astype(out.dtype)


def interact_near(slots, weights, extra, combined, *outs):
    for slot, out in zip(slots, outs):
        out[...] = field_of(weights, extra, combined, slot).astype(out.dtype)


def local(source, operators, mie_factor, pair_source, pair_class, pair_scale):
    rows, spheres = source.shape
    classes, full, _ = operators.shape
    visits = pair_source.shape[0]
    groups = full // rows
    blocks = lax.axis_size("blk")
    visiting = [source]
    for s in range(1, visits):
        visiting.append(lax.ppermute(source, "blk", [(b, (b + s) % blocks) for b in range(blocks)]))

    units = (pair_scale.astype(jnp.float32) * SCALE_UNIT).astype(jnp.int32)
    codes = (pair_class * 2**SPHERE_BITS + pair_source) * 2**SCALE_BITS + units
    table, weights, extra = pl.pallas_call(
        prepare,
        out_shape=(
            jax.ShapeDtypeStruct((classes, visits, spheres, spheres), jnp.bfloat16),
            jax.ShapeDtypeStruct((classes, full, DEPTH), jnp.bfloat16),
            jax.ShapeDtypeStruct((full, LEAD * classes), jnp.bfloat16),
        ),
        in_specs=[VMEM, pl.BlockSpec(memory_space=pl.ANY)],
        out_specs=(VMEM,) * 3,
        scratch_shapes=[
            pltpu.VMEM((classes, full, full), jnp.bfloat16),
            pltpu.SemaphoreType.DMA((classes,)),
        ],
        compiler_params=pltpu.CompilerParams(vmem_limit_bytes=40 * 2**20),
        cost_estimate=pl.CostEstimate(
            flops=2 * classes * full * full * rows, bytes_accessed=2 * operators.size, transcendentals=0
        ),
        name="prepare",
    )(codes, operators)

    def call(kernel, out_shape, flops, *operands):
        return pl.pallas_call(
            kernel,
            out_shape=out_shape,
            in_specs=[VMEM] * len(operands),
            out_specs=jax.tree.map(lambda _: VMEM, out_shape),
            compiler_params=pltpu.CompilerParams(vmem_limit_bytes=16 * 2**20),
            cost_estimate=pl.CostEstimate(flops=flops, bytes_accessed=2 * source.size, transcendentals=0),
        )(*operands)

    def shape(dtype, *lead):
        return jax.ShapeDtypeStruct((*lead, rows, spheres), dtype)

    gather = 2 * rows * spheres * spheres * classes
    product = 2 * rows * rows * spheres * classes
    late = max(visits - EARLY, 0)
    early = call(gather_early, shape(jnp.float32, classes), (visits - late) * gather, *visiting[:EARLY], table)

    def exchange(x, distance):
        return lax.ppermute(x, "deg", [(i, i ^ distance) for i in range(groups)])

    far, near = (3,), (2, 1, 0)
    combined, crossed = call(
        functools.partial(interact_far, EARLY, far),
        (jax.ShapeDtypeStruct((classes, LEAD + DEPTH, spheres), jnp.bfloat16), shape(jnp.bfloat16)),
        late * gather + len(far) * product,
        early,
        *visiting[EARLY:],
        table,
        weights,
        extra,
    )
    crossed = exchange(crossed, 1)
    ahead, beside, field = call(
        functools.partial(interact_near, near),
        (shape(jnp.float32), shape(jnp.bfloat16), shape(jnp.float32)),
        len(near) * product,
        weights,
        extra,
        combined,
    )
    ahead = exchange((ahead + crossed.astype(jnp.float32)).astype(jnp.bfloat16), 2)
    beside = exchange(beside, 1)
    field = field + beside.astype(jnp.float32) + ahead.astype(jnp.float32)
    return source.astype(jnp.float32) - mie_factor * field


def solution(mesh):
    return jax.shard_map(
        local,
        mesh=mesh,
        in_specs=(
            P("deg", "blk"),
            P(),
            P("deg", "blk"),
            P(None, None, "blk"),
            P(None, None, "blk"),
            P(None, None, "blk"),
        ),
        out_specs=P("deg", "blk"),
        check_vma=False,
    )
```

```python
import functools

import jax
import jax.numpy as jnp
from jax import lax
from jax.experimental import pallas as pl
from jax.experimental.pallas import tpu as pltpu
from jax.sharding import PartitionSpec as P


LANES = 128
STRIP = 64
ORDER = (0, 1, 2, 3, 4, 5)
EARLY = 4
SPHERE_BITS = 8
SCALE_BITS = 10
SCALE_UNIT = 512
DEPTH = 256
LEAD = 8
VMEM = pl.BlockSpec(memory_space=pltpu.VMEM)


def column_windows(full, rows):
    windows = []
    for d in range(full // rows):
        start = d * rows // LANES * LANES
        if (d + 1) * rows - start > DEPTH:
            start += LANES
        windows.append((start, min(DEPTH, full - start), d * rows - start))
        assert windows[-1][2] >= -LEAD and windows[-1][2] % 8 == 0
    return windows


def prepare(codes, operators, table, weights, extra, stage, arrived):
    classes, full, _ = operators.shape
    visits, slots, spheres = codes.shape
    rows = full // lax.axis_size("deg")
    deg = lax.axis_index("deg")
    windows = column_windows(full, rows)

    def window(d, c):
        start, length, _ = windows[d]
        if length == DEPTH:
            return pltpu.make_async_copy(operators.at[c, :, start : start + length], weights.at[c], arrived.at[c])
        return pltpu.make_async_copy(operators.at[c], stage.at[c], arrived.at[c])

    def each_group(body):
        for d in range(full // rows):
            pl.when(deg == d)(functools.partial(body, d))

    def fetch(d):
        for c in range(classes):
            window(d, c).start()

    each_group(fetch)

    def spread(x):
        return [jnp.broadcast_to(x[k : k + 1, :], (LEAD, spheres)) for k in range(slots)]

    def strip(tile):
        return jnp.concatenate([tile] * (STRIP // LEAD), axis=0)

    zero = jnp.zeros((), jnp.bfloat16)
    sphere = lax.broadcasted_iota(jnp.int32, (STRIP, spheres), 0).astype(jnp.float32).astype(jnp.bfloat16)

    def tables(s, _):
        kind = jnp.right_shift(codes[s], SPHERE_BITS + SCALE_BITS)
        picked = jnp.bitwise_and(jnp.right_shift(codes[s], SCALE_BITS), 2**SPHERE_BITS - 1)
        scale = jnp.bitwise_and(codes[s], 2**SCALE_BITS - 1).astype(jnp.float32) * (1.0 / SCALE_UNIT)
        picked = [strip(x) for x in spread(picked.astype(jnp.float32).astype(jnp.bfloat16))]
        scale = [strip(x) for x in spread(scale.astype(jnp.bfloat16))]
        kind = spread(kind.astype(jnp.float32).astype(jnp.bfloat16))
        one = jnp.ones((), jnp.bfloat16)
        mine = [[strip(jnp.where(x == jnp.asarray(c, x.dtype), one, zero)) for x in kind] for c in range(classes)]
        for start in range(0, spheres, STRIP):
            here = sphere + jnp.asarray(start, jnp.bfloat16)
            hits = [jnp.where(here == picked[k], scale[k], zero) for k in range(slots)]
            for c in range(classes):
                terms = [hits[k] * mine[c][k] for k in range(slots)]
                while len(terms) > 1:
                    terms = [sum(terms[i + 1 : i + 2], terms[i]) for i in range(0, len(terms), 2)]
                table[c, s, start : start + STRIP] = terms[0]
        return 0

    lax.fori_loop(0, visits, tables, 0)

    def finish(d):
        start, length, first_row = windows[d]
        whole = length // LANES * LANES
        row = lax.broadcasted_iota(jnp.int32, (LANES, extra.shape[1]), 0) - (LANES + first_row)
        column = lax.broadcasted_iota(jnp.int32, (LANES, extra.shape[1]), 1)
        before = None
        for c in range(classes):
            window(d, c).wait()
            if length < DEPTH:
                weights[c, :, :whole] = stage[c, :, start : start + whole]
                weights[c, :, whole:] = jnp.zeros((full, DEPTH - whole), jnp.bfloat16)
                weights[c, :, whole:length] = stage[c, :, start + whole : start + length]
            if first_row < 0:
                pick = jnp.where((row >= 0) & (row + LEAD * c == column), 1.0, 0.0).astype(jnp.bfloat16)
                term = jnp.dot(stage[c, :, start - LANES : start], pick, preferred_element_type=jnp.float32)
                before = term if before is None else before + term
        extra[...] = jnp.zeros_like(extra) if before is None else before.astype(jnp.bfloat16)

    each_group(finish)


def add_visits(start, visiting, table, visits, c):
    for s, block in zip(visits, visiting):
        term = jnp.dot(block[...], table[c, s], preferred_element_type=jnp.float32)
        start = term if start is None else start + term
    return start


def gather_early(visits, *refs):
    *visiting, table, early = refs
    for c in range(table.shape[0]):
        early[c] = add_visits(None, visiting, table, visits, c)


def field_of(weights, extra, combined, slot):
    rows = extra.shape[0] // lax.axis_size("deg")
    chunk = pl.ds(pl.multiple_of(jnp.bitwise_xor(lax.axis_index("deg"), slot) * rows, 8), rows)
    lead = jnp.concatenate([combined[c, :LEAD] for c in range(weights.shape[0])], axis=0)
    field = jnp.dot(extra[chunk], lead, preferred_element_type=jnp.float32)
    for c in range(weights.shape[0]):
        field += jnp.dot(weights[c, chunk], combined[c, LEAD:], preferred_element_type=jnp.float32)
    return field


def interact_far(visits, slots, *refs):
    early, *visiting, table, weights, extra, combined = refs[: len(refs) - len(slots)]
    rows = early.shape[1]
    place = jnp.int32(LEAD)
    for d, (_, _, first_row) in enumerate(column_windows(weights.shape[1], rows)):
        place += jnp.where(lax.axis_index("deg") == d, first_row, 0)
    combined[...] = jnp.zeros_like(combined)
    for c in range(table.shape[0]):
        mixed = add_visits(early[c], visiting, table, visits, c)
        combined[c, pl.ds(pl.multiple_of(place, 8), rows)] = mixed.astype(jnp.bfloat16)
    for slot, out in zip(slots, refs[len(refs) - len(slots) :]):
        out[...] = field_of(weights, extra, combined, slot).astype(out.dtype)


def interact_near(slots, weights, extra, combined, *outs):
    for slot, out in zip(slots, outs):
        out[...] = field_of(weights, extra, combined, slot).astype(out.dtype)


def local(source, operators, mie_factor, pair_source, pair_class, pair_scale):
    rows, spheres = source.shape
    classes, full, _ = operators.shape
    visits = pair_source.shape[0]
    groups = full // rows
    blocks = lax.axis_size("blk")
    visiting = [source]
    for s in range(1, visits):
        visiting.append(lax.ppermute(source, "blk", [(b, (b + s) % blocks) for b in range(blocks)]))

    units = (pair_scale.astype(jnp.float32) * SCALE_UNIT).astype(jnp.int32)
    codes = (pair_class * 2**SPHERE_BITS + pair_source) * 2**SCALE_BITS + units
    table, weights, extra = pl.pallas_call(
        prepare,
        out_shape=(
            jax.ShapeDtypeStruct((classes, visits, spheres, spheres), jnp.bfloat16),
            jax.ShapeDtypeStruct((classes, full, DEPTH), jnp.bfloat16),
            jax.ShapeDtypeStruct((full, LEAD * classes), jnp.bfloat16),
        ),
        in_specs=[VMEM, pl.BlockSpec(memory_space=pl.ANY)],
        out_specs=(VMEM,) * 3,
        scratch_shapes=[
            pltpu.VMEM((classes, full, full), jnp.bfloat16),
            pltpu.SemaphoreType.DMA((classes,)),
        ],
        compiler_params=pltpu.CompilerParams(vmem_limit_bytes=40 * 2**20),
        cost_estimate=pl.CostEstimate(
            flops=2 * classes * full * full * rows, bytes_accessed=2 * operators.size, transcendentals=0
        ),
        name="prepare",
    )(codes, operators)

    def call(kernel, out_shape, flops, *operands):
        return pl.pallas_call(
            kernel,
            out_shape=out_shape,
            in_specs=[VMEM] * len(operands),
            out_specs=jax.tree.map(lambda _: VMEM, out_shape),
            compiler_params=pltpu.CompilerParams(vmem_limit_bytes=16 * 2**20),
            cost_estimate=pl.CostEstimate(flops=flops, bytes_accessed=2 * source.size, transcendentals=0),
        )(*operands)

    def shape(dtype, *lead):
        return jax.ShapeDtypeStruct((*lead, rows, spheres), dtype)

    gather = 2 * rows * spheres * spheres * classes
    product = 2 * rows * rows * spheres * classes
    first, late = ORDER[:EARLY], ORDER[EARLY:]
    early = call(
        functools.partial(gather_early, first),
        shape(jnp.float32, classes),
        len(first) * gather,
        *(visiting[s] for s in first),
        table,
    )

    def exchange(x, distance):
        return lax.ppermute(x, "deg", [(i, i ^ distance) for i in range(groups)])

    far, near = (3,), (2, 1, 0)
    combined, crossed = call(
        functools.partial(interact_far, late, far),
        (jax.ShapeDtypeStruct((classes, LEAD + DEPTH, spheres), jnp.bfloat16), shape(jnp.bfloat16)),
        len(late) * gather + len(far) * product,
        early,
        *(visiting[s] for s in late),
        table,
        weights,
        extra,
    )
    crossed = exchange(crossed, 1)
    ahead, beside, field = call(
        functools.partial(interact_near, near),
        (shape(jnp.float32), shape(jnp.bfloat16), shape(jnp.float32)),
        len(near) * product,
        weights,
        extra,
        combined,
    )
    ahead = exchange((ahead + crossed.astype(jnp.float32)).astype(jnp.bfloat16), 2)
    beside = exchange(beside, 1)
    field = field + beside.astype(jnp.float32) + ahead.astype(jnp.float32)
    return source.astype(jnp.float32) - mie_factor * field


def solution(mesh):
    return jax.shard_map(
        local,
        mesh=mesh,
        in_specs=(
            P("deg", "blk"),
            P(),
            P("deg", "blk"),
            P(None, None, "blk"),
            P(None, None, "blk"),
            P(None, None, "blk"),
        ),
        out_specs=P("deg", "blk"),
        check_vma=False,
    )
```

```python
import functools

import jax
import jax.numpy as jnp
from jax import lax
from jax.experimental import pallas as pl
from jax.experimental.pallas import tpu as pltpu
from jax.sharding import PartitionSpec as P


LANES = 128
STRIP = 32
ORDER = (0, 1, 3, 2, 4, 5)
EARLY = 3
SPHERE_BITS = 8
SCALE_BITS = 10
SCALE_UNIT = 512
DEPTH = 256
LEAD = 8
VMEM = pl.BlockSpec(memory_space=pltpu.VMEM)


def column_windows(full, rows):
    windows = []
    for d in range(full // rows):
        start = d * rows // LANES * LANES
        if (d + 1) * rows - start > DEPTH:
            start += LANES
        windows.append((start, min(DEPTH, full - start), d * rows - start))
        assert windows[-1][2] >= -LEAD and windows[-1][2] % 8 == 0
    return windows


def prepare(codes, operators, table, weights, extra, stage, arrived):
    classes, full, _ = operators.shape
    visits, slots, spheres = codes.shape
    rows = full // lax.axis_size("deg")
    deg = lax.axis_index("deg")
    windows = column_windows(full, rows)

    def window(d, c):
        start, length, _ = windows[d]
        if length == DEPTH:
            return pltpu.make_async_copy(operators.at[c, :, start : start + length], weights.at[c], arrived.at[c])
        return pltpu.make_async_copy(operators.at[c], stage.at[c], arrived.at[c])

    def each_group(body):
        for d in range(full // rows):
            pl.when(deg == d)(functools.partial(body, d))

    def fetch(d):
        for c in range(classes):
            window(d, c).start()

    each_group(fetch)

    def spread(x):
        return [jnp.broadcast_to(x[k : k + 1, :], (LEAD, spheres)) for k in range(slots)]

    def strip(tile):
        return jnp.concatenate([tile] * (STRIP // LEAD), axis=0)

    zero = jnp.zeros((), jnp.bfloat16)
    sphere = lax.broadcasted_iota(jnp.int32, (STRIP, spheres), 0).astype(jnp.float32).astype(jnp.bfloat16)

    def tables(s, _):
        kind = jnp.right_shift(codes[s], SPHERE_BITS + SCALE_BITS)
        picked = jnp.bitwise_and(jnp.right_shift(codes[s], SCALE_BITS), 2**SPHERE_BITS - 1)
        scale = jnp.bitwise_and(codes[s], 2**SCALE_BITS - 1).astype(jnp.float32) * (1.0 / SCALE_UNIT)
        picked = [strip(x) for x in spread(picked.astype(jnp.float32).astype(jnp.bfloat16))]
        scale = [strip(x) for x in spread(scale.astype(jnp.bfloat16))]
        kind = spread(kind.astype(jnp.float32).astype(jnp.bfloat16))
        one = jnp.ones((), jnp.bfloat16)
        mine = [[strip(jnp.where(x == jnp.asarray(c, x.dtype), one, zero)) for x in kind] for c in range(classes)]
        for start in range(0, spheres, STRIP):
            here = sphere + jnp.asarray(start, jnp.bfloat16)
            hits = [jnp.where(here == picked[k], scale[k], zero) for k in range(slots)]
            for c in range(classes):
                terms = [hits[k] * mine[c][k] for k in range(slots)]
                while len(terms) > 1:
                    terms = [sum(terms[i + 1 : i + 2], terms[i]) for i in range(0, len(terms), 2)]
                table[c, s, start : start + STRIP] = terms[0]
        return 0

    lax.fori_loop(0, visits, tables, 0)

    def finish(d):
        start, length, first_row = windows[d]
        whole = length // LANES * LANES
        row = lax.broadcasted_iota(jnp.int32, (LANES, extra.shape[1]), 0) - (LANES + first_row)
        column = lax.broadcasted_iota(jnp.int32, (LANES, extra.shape[1]), 1)
        before = None
        for c in range(classes):
            window(d, c).wait()
            if length < DEPTH:
                weights[c, :, :whole] = stage[c, :, start : start + whole]
                weights[c, :, whole:] = jnp.zeros((full, DEPTH - whole), jnp.bfloat16)
                weights[c, :, whole:length] = stage[c, :, start + whole : start + length]
            if first_row < 0:
                pick = jnp.where((row >= 0) & (row + LEAD * c == column), 1.0, 0.0).astype(jnp.bfloat16)
                term = jnp.dot(stage[c, :, start - LANES : start], pick, preferred_element_type=jnp.float32)
                before = term if before is None else before + term
        extra[...] = jnp.zeros_like(extra) if before is None else before.astype(jnp.bfloat16)

    each_group(finish)


def add_visits(start, visiting, table, visits, c):
    for s, block in zip(visits, visiting):
        term = jnp.dot(block[...], table[c, s], preferred_element_type=jnp.float32)
        start = term if start is None else start + term
    return start


def gather_early(visits, *refs):
    *visiting, table, early = refs
    for c in range(table.shape[0]):
        early[c] = add_visits(None, visiting, table, visits, c)


def field_of(weights, extra, combined, slot):
    rows = extra.shape[0] // lax.axis_size("deg")
    chunk = pl.ds(pl.multiple_of(jnp.bitwise_xor(lax.axis_index("deg"), slot) * rows, 8), rows)
    lead = jnp.concatenate([combined[c, :LEAD] for c in range(weights.shape[0])], axis=0)
    field = jnp.dot(extra[chunk], lead, preferred_element_type=jnp.float32)
    for c in range(weights.shape[0]):
        field += jnp.dot(weights[c, chunk], combined[c, LEAD:], preferred_element_type=jnp.float32)
    return field


def interact_far(visits, slots, *refs):
    early, *visiting, table, weights, extra, combined = refs[: len(refs) - len(slots)]
    rows = early.shape[1]
    place = jnp.int32(LEAD)
    for d, (_, _, first_row) in enumerate(column_windows(weights.shape[1], rows)):
        place += jnp.where(lax.axis_index("deg") == d, first_row, 0)
    combined[...] = jnp.zeros_like(combined)
    for c in range(table.shape[0]):
        mixed = add_visits(early[c], visiting, table, visits, c)
        combined[c, pl.ds(pl.multiple_of(place, 8), rows)] = mixed.astype(jnp.bfloat16)
    for slot, out in zip(slots, refs[len(refs) - len(slots) :]):
        out[...] = field_of(weights, extra, combined, slot).astype(out.dtype)


def interact_near(slots, weights, extra, combined, *outs):
    for slot, out in zip(slots, outs):
        out[...] = field_of(weights, extra, combined, slot).astype(out.dtype)


def local(source, operators, mie_factor, pair_source, pair_class, pair_scale):
    rows, spheres = source.shape
    classes, full, _ = operators.shape
    visits = pair_source.shape[0]
    groups = full // rows
    blocks = lax.axis_size("blk")
    visiting = [source]
    for s in range(1, visits):
        visiting.append(lax.ppermute(source, "blk", [(b, (b + s) % blocks) for b in range(blocks)]))

    units = (pair_scale.astype(jnp.float32) * SCALE_UNIT).astype(jnp.int32)
    codes = (pair_class * 2**SPHERE_BITS + pair_source) * 2**SCALE_BITS + units
    table, weights, extra = pl.pallas_call(
        prepare,
        out_shape=(
            jax.ShapeDtypeStruct((classes, visits, spheres, spheres), jnp.bfloat16),
            jax.ShapeDtypeStruct((classes, full, DEPTH), jnp.bfloat16),
            jax.ShapeDtypeStruct((full, LEAD * classes), jnp.bfloat16),
        ),
        in_specs=[VMEM, pl.BlockSpec(memory_space=pl.ANY)],
        out_specs=(VMEM,) * 3,
        scratch_shapes=[
            pltpu.VMEM((classes, full, full), jnp.bfloat16),
            pltpu.SemaphoreType.DMA((classes,)),
        ],
        compiler_params=pltpu.CompilerParams(vmem_limit_bytes=40 * 2**20),
        cost_estimate=pl.CostEstimate(
            flops=2 * classes * full * full * rows, bytes_accessed=2 * operators.size, transcendentals=0
        ),
        name="prepare",
    )(codes, operators)

    def call(kernel, out_shape, flops, *operands):
        return pl.pallas_call(
            kernel,
            out_shape=out_shape,
            in_specs=[VMEM] * len(operands),
            out_specs=jax.tree.map(lambda _: VMEM, out_shape),
            compiler_params=pltpu.CompilerParams(vmem_limit_bytes=16 * 2**20),
            cost_estimate=pl.CostEstimate(flops=flops, bytes_accessed=2 * source.size, transcendentals=0),
        )(*operands)

    def shape(dtype, *lead):
        return jax.ShapeDtypeStruct((*lead, rows, spheres), dtype)

    gather = 2 * rows * spheres * spheres * classes
    product = 2 * rows * rows * spheres * classes
    first, late = ORDER[:EARLY], ORDER[EARLY:]
    early = call(
        functools.partial(gather_early, first),
        shape(jnp.float32, classes),
        len(first) * gather,
        *(visiting[s] for s in first),
        table,
    )

    def exchange(x, distance):
        return lax.ppermute(x, "deg", [(i, i ^ distance) for i in range(groups)])

    far, near = (3,), (2, 1, 0)
    combined, crossed = call(
        functools.partial(interact_far, late, far),
        (jax.ShapeDtypeStruct((classes, LEAD + DEPTH, spheres), jnp.bfloat16), shape(jnp.bfloat16)),
        len(late) * gather + len(far) * product,
        early,
        *(visiting[s] for s in late),
        table,
        weights,
        extra,
    )
    crossed = exchange(crossed, 1)
    ahead, beside, field = call(
        functools.partial(interact_near, near),
        (shape(jnp.float32), shape(jnp.bfloat16), shape(jnp.float32)),
        len(near) * product,
        weights,
        extra,
        combined,
    )
    ahead = exchange((ahead + crossed.astype(jnp.float32)).astype(jnp.bfloat16), 2)
    beside = exchange(beside, 1)
    field = field + beside.astype(jnp.float32) + ahead.astype(jnp.float32)
    return source.astype(jnp.float32) - mie_factor * field


def solution(mesh):
    return jax.shard_map(
        local,
        mesh=mesh,
        in_specs=(
            P("deg", "blk"),
            P(),
            P("deg", "blk"),
            P(None, None, "blk"),
            P(None, None, "blk"),
            P(None, None, "blk"),
        ),
        out_specs=P("deg", "blk"),
        check_vma=False,
    )
```
